256 devices in a mesh: dp: 32 (over x_lo, z, core), mp: 8 (over x_hi, y).
Axes of the slice: x: 4 (x_hi: 2, x_lo: 2; x = x_hi * 2 + x_lo), y: 4, z: 8, core: 2. Of those that a mesh axis runs over, the one named last changes fastest.
Arguments:
- token_ids: int32 [32, 512], P('dp', 'mp'), may hold values from 0 to 128255
- embedding: bfloat16 [128256, 8192], P('mp', 'dp'), may hold values from -6 to 6
- norm_gain: bfloat16 [8192], replicated, may hold values from 0.099609375 to 1.8984375
- query_weight: bfloat16 [8192, 4096], P('dp', 'mp'), may hold values from -4 to 4
- key_weight: bfloat16 [8192, 1024], P('dp', 'mp'), may hold values from -0.0625 to 0.0625
- value_weight: bfloat16 [8192, 1024], P('dp', 'mp'), may hold values from -0.0625 to 0.0625
Outputs:
- attention: bfloat16 [16384, 4096], P('dp', 'mp')
The draws below stay inside these ranges and needn't reach their ends.
All inputs are finite; a program needn't handle non-finite values.
Results may differ from the reference program's by a relative error of at most 0.0095.
The reference program's roundings to bfloat16 on the way (of `embedded`, `normed` and `weights`) count: a program that leaves them out, or rounds other values in their place, can miss the bound.
Values may be sent and summed in bfloat16 or wider, within the bound.
No kernel may reach another device: no remote copies, remote signals or barrier semaphores. Data moves between devices by JAX's collectives and lax.ppermute only.
A program may use at most 128 MiB of HBM per device.

```python
import math
import jax
import jax.numpy as jnp
import numpy as np
from jax import lax

D = 8192
VOCAB = 128256
HD = 128
KVH = 8
HQ = 32
SEQ = 512
RESPONSES = 32


def draw_query_weight(key, part):
    first_key = jax.random.fold_in(jax.random.fold_in(key, 17), 0)
    values = jnp.clip(jax.random.normal(first_key, (D, HQ * HD), jnp.float32), -6.0, 6.0) * D ** (-0.5)
    values = jnp.clip(values, -4.0, 4.0)
    return values.astype(jnp.bfloat16)


def plant(result, rng, least, high):
    extent = result.shape
    place = [jax.random.randint(jax.random.fold_in(rng, axis), (), 0, extent[axis]) for axis in range(len(extent))]
    result = result.at[tuple(place)].set(least)
    longest = extent.index(max(extent))
    place[longest] = (place[longest] + 1) % extent[longest]
    return result.at[tuple(place)].set(high)


def levels(own_key, extent, cuts, smallest, high):
    factor_of = 1.0
    for dim, parts in cuts:
        heights = jax.random.uniform(jax.random.fold_in(jax.random.fold_in(own_key, 6), dim), (parts,), jnp.float32, smallest / len(cuts), high / len(cuts))
        factor_of = factor_of * jnp.repeat(jnp.exp(heights), extent[dim] // parts).reshape((-1,) + (1,) * (len(extent) - 1 - dim))
    return factor_of


def ranked_wide(stream_key, extent, amount, skew):
    loads = [min(1 << octave, amount + 1 - (1 << octave)) * (1 << 20) // math.isqrt((1 << octave) ** skew) + 1 for octave in range((amount + 1).bit_length()) if 1 << octave <= amount]
    spread = 1 + sum(loads) // (1 << 30)
    grid = np.cumsum(np.array([max(1, weight // spread) for weight in loads]))
    lot = jax.random.randint(jax.random.fold_in(stream_key, 1), extent, 0, int(grid[len(loads) - 1]))
    start = jnp.left_shift(1, jnp.searchsorted(jnp.asarray(grid, jnp.int32), lot, side="right").astype(jnp.int32))
    standing = start - 1 + jax.random.randint(jax.random.fold_in(stream_key, 4), extent, 0, 1 << 30) % jnp.minimum(start, amount + 1 - start)
    return jax.random.permutation(jax.random.fold_in(stream_key, 2), amount)[standing].astype(jnp.int32)


def bell_draw(rng, dims, scale, reach, cuts=(), kind=jnp.bfloat16):
    result = scale * jax.random.normal(rng, dims, jnp.float32)
    if cuts:
        result = result * levels(rng, dims, cuts, -0.22, 0.18)
    return jnp.clip(result, -reach, reach).astype(kind)


def setup_inputs(seed: int = 0) -> dict:
    seeds = jax.random.split(jax.random.key(seed), 7)
    token_ids = plant(ranked_wide(seeds[0], (RESPONSES, SEQ), VOCAB, 2), jax.random.fold_in(seeds[0], 3), 0, VOCAB - 1).astype(jnp.int32)
    embedding = bell_draw(seeds[1], (VOCAB, D), 1.0, 6.0, ((0, 8), (1, 32)))
    norm_gain = jnp.clip(1.0 + 0.18 * jax.random.normal(seeds[2], (D,), jnp.float32), 0.099609375, 1.8984375).astype(jnp.bfloat16)
    query_weight = draw_query_weight(jax.random.fold_in(seeds[6], 71), 0)
    key_weight = bell_draw(seeds[4], (D, KVH * HD), D ** -0.5, 0.0625, ((0, 32), (1, 8)))
    value_weight = bell_draw(seeds[5], (D, KVH * HD), D ** -0.5, 0.0625, ((0, 32), (1, 8)))
    return dict(token_ids=token_ids, embedding=embedding, norm_gain=norm_gain, query_weight=query_weight, key_weight=key_weight, value_weight=value_weight)


rope_base = 500000.0
epsilon = 1e-05

def normalize(values, norm_gain):
    factor = lax.rsqrt(lax.optimization_barrier(jnp.mean(values * values, axis=-1, keepdims=True)) + epsilon)
    return (values * factor * norm_gain.astype(jnp.float32)).astype(jnp.bfloat16)

def rotate(values, positions):
    half_width = values.shape[-1] // 2
    frequency = rope_base ** (-(jnp.arange(half_width, dtype=jnp.float32) * 2.0) / values.shape[-1])
    angles = (positions[:, None] * frequency[None, :])[:, None, :]
    cosine = jnp.cos(angles)
    sine_wave = jnp.sin(angles)
    first_half = values[..., :half_width]
    second_half = values[..., half_width:]
    return jnp.concatenate([first_half * cosine - second_half * sine_wave, second_half * cosine + first_half * sine_wave], axis=-1)

def attend(queries, key_block, value_block):
    length = queries.shape[0]
    scores = jnp.einsum('skgd,tkd->kgst', queries.astype(jnp.float32), key_block.astype(jnp.float32)) * queries.shape[-1] ** (-0.5)
    causal = jnp.arange(length)[:, None] >= jnp.arange(length)[None, :]
    scores = jnp.where(causal, scores, -jnp.inf)
    highest = lax.optimization_barrier(jnp.max(scores, axis=-1, keepdims=True))
    raised = jnp.exp(scores - highest)
    weights = (raised / lax.optimization_barrier(jnp.sum(raised, axis=-1, keepdims=True))).astype(jnp.bfloat16)
    blended = jnp.einsum('kgst,tkd->skgd', weights.astype(jnp.float32), value_block.astype(jnp.float32))
    return blended.reshape(length, -1).astype(jnp.bfloat16)

def reference(token_ids, embedding, norm_gain, query_weight, key_weight, value_weight):
    response_count = token_ids.shape[0]
    length = token_ids.shape[1]
    flat_ids = token_ids.reshape(-1).astype(jnp.int32)
    embedded = jnp.take(embedding, flat_ids, axis=0).astype(jnp.float32)
    normed = normalize(embedded, norm_gain)
    query_proj = jnp.dot(normed, query_weight, preferred_element_type=jnp.float32)
    key_proj = jnp.dot(normed, key_weight, preferred_element_type=jnp.float32)
    value_proj = jnp.dot(normed, value_weight, preferred_element_type=jnp.float32)
    positions = jnp.arange(length, dtype=jnp.float32)
    queries = rotate(query_proj.reshape(response_count, length, HQ, HD), positions).astype(jnp.bfloat16)
    queries = queries.reshape(response_count, length, KVH, HQ // KVH, HD)
    key_block = rotate(key_proj.reshape(response_count, length, KVH, HD), positions).astype(jnp.bfloat16)
    value_block = value_proj.reshape(response_count, length, KVH, HD).astype(jnp.bfloat16)
    output = lax.map(lambda group: attend(group[0], group[1], group[2]), (queries, key_block, value_block))
    return output.reshape(response_count * length, HQ * HD)
```

```python
import jax
import jax.numpy as jnp
from jax import lax
from jax.sharding import Mesh
from jax.sharding import PartitionSpec as P

HD = 128
DP = ("xl", "z", "c")
MP = ("xh", "y")
ALL = DP + MP

rope_base = 500000.0
epsilon = 1e-05
SLOTS = 512


def running_count(flags):
    rows, length = flags.shape
    chunk = 128
    ones = flags.astype(jnp.bfloat16).reshape(rows, length // chunk, chunk)
    upto = (jnp.arange(chunk)[:, None] <= jnp.arange(chunk)[None, :]).astype(jnp.bfloat16)
    within = jnp.einsum("rnc,cd->rnd", ones, upto, preferred_element_type=jnp.float32)
    total = within[..., -1]
    n = length // chunk
    before = (jnp.arange(n)[:, None] < jnp.arange(n)[None, :]).astype(jnp.bfloat16)
    offset = jnp.einsum(
        "rn,nk->rk", total.astype(jnp.bfloat16), before, preferred_element_type=jnp.float32
    )
    return (within + offset[..., None]).astype(jnp.int32).reshape(rows, length)


def look_up(embedding, every_id):
    dp_count, mp_count, span = every_id.shape
    vocab_rows, columns = embedding.shape
    me = lax.axis_index(MP)
    by_span = every_id.transpose(1, 0, 2).reshape(mp_count, dp_count * span)
    local = by_span - me * vocab_rows
    inside = (local >= 0) & (local < vocab_rows)
    rank = jnp.where(inside, running_count(inside) - 1, -1)
    mine = lax.dynamic_index_in_dim(by_span, me, 0, keepdims=False)
    bounds = jnp.arange(mp_count)[:, None] * vocab_rows
    of_shard = (mine[None, :] >= bounds) & (mine[None, :] < bounds + vocab_rows)
    counted = running_count(of_shard)
    place = jnp.sum(jnp.where(of_shard, counted - 1, 0), axis=0)
    shard = jnp.sum(jnp.where(of_shard, jnp.arange(mp_count)[:, None], 0), axis=0)
    starts = jnp.arange(mp_count)[:, None, None] * vocab_rows
    held = (by_span[None] >= starts) & (by_span[None] < starts + vocab_rows)
    most = jnp.max(jnp.sum(held.astype(jnp.int32), axis=-1))
    rounds = (most + SLOTS - 1) // SLOTS

    def exchange(turn):
        wanted = turn * SLOTS + jnp.arange(SLOTS)
        rows = jnp.sum(
            jnp.where(rank[:, None, :] == wanted[None, :, None], local[:, None, :], 0), axis=-1
        )
        sent = jnp.take(embedding, rows.reshape(-1), axis=0, mode="clip")
        got = lax.all_to_all(
            sent.reshape(mp_count, SLOTS, columns), MP, split_axis=0, concat_axis=0, tiled=True
        )
        slot = place - turn * SLOTS
        at = shard * SLOTS + jnp.clip(slot, 0, SLOTS - 1)
        return jnp.take(got.reshape(-1, columns), at, axis=0, mode="clip"), slot

    found, _ = exchange(0)

    def more(state):
        turn, found = state
        rows, slot = exchange(turn)
        ours = (slot >= 0) & (slot < SLOTS)
        return turn + 1, jnp.where(ours[:, None], rows, found)

    _, found = lax.while_loop(lambda state: state[0] < rounds, more, (jnp.int32(1), found))
    return found


def normalize(values, norm_gain):
    factor = lax.rsqrt(jnp.mean(values * values, axis=-1, keepdims=True) + epsilon)
    return (values * factor * norm_gain.astype(jnp.float32)).astype(jnp.bfloat16)


def rotate(values, positions):
    half_width = values.shape[-1] // 2
    frequency = rope_base ** (-(jnp.arange(half_width, dtype=jnp.float32) * 2.0) / values.shape[-1])
    angles = (positions[:, None] * frequency[None, :])[:, None, :]
    cosine = jnp.cos(angles)
    sine_wave = jnp.sin(angles)
    first_half = values[..., :half_width]
    second_half = values[..., half_width:]
    return jnp.concatenate(
        [
            first_half * cosine - second_half * sine_wave,
            second_half * cosine + first_half * sine_wave,
        ],
        axis=-1,
    )


def attend(queries, key_block, value_block):
    length = queries.shape[0]
    scores = jnp.einsum(
        "skgd,tkd->kgst", queries, key_block, preferred_element_type=jnp.float32
    ) * queries.shape[-1] ** (-0.5)
    causal = jnp.arange(length)[:, None] >= jnp.arange(length)[None, :]
    scores = jnp.where(causal, scores, -jnp.inf)
    highest = jnp.max(scores, axis=-1, keepdims=True)
    raised = jnp.exp(scores - highest)
    weights = (raised / jnp.sum(raised, axis=-1, keepdims=True)).astype(jnp.bfloat16)
    blended = jnp.einsum("kgst,tkd->skgd", weights, value_block, preferred_element_type=jnp.float32)
    return blended.reshape(length, -1).astype(jnp.bfloat16)


def per_device(token_ids, embedding, norm_gain, query_weight, key_weight, value_weight):
    responses, span = token_ids.shape
    dp_count = lax.axis_size(DP)
    mp_count = lax.axis_size(MP)
    length = span * mp_count
    weights = lax.all_gather(
        jnp.concatenate([query_weight, key_weight, value_weight], axis=1), DP, axis=0, tiled=True
    )
    copies = jnp.broadcast_to(token_ids, (dp_count * mp_count, span))
    every_id = lax.all_to_all(copies, ALL, split_axis=0, concat_axis=0, tiled=True)
    found = look_up(embedding, every_id.reshape(dp_count, mp_count, span))
    found, weights = lax.optimization_barrier((found, weights))
    moved = lax.all_to_all(
        found.reshape(dp_count, span, -1), DP, split_axis=0, concat_axis=0, tiled=True
    )
    share = moved.transpose(1, 0, 2).reshape(span, -1).astype(jnp.float32)
    flat_normed = lax.all_gather(normalize(share, norm_gain), MP, axis=0, tiled=True)

    projected = jnp.dot(flat_normed, weights, preferred_element_type=jnp.float32)
    q_width, k_width = query_weight.shape[1], key_weight.shape[1]
    heads_here, kv_here = q_width // HD, k_width // HD
    positions = jnp.arange(length, dtype=jnp.float32)
    queries = rotate(projected[:, :q_width].reshape(length, heads_here, HD), positions)
    queries = queries.astype(jnp.bfloat16).reshape(length, kv_here, heads_here // kv_here, HD)
    key_block = rotate(
        projected[:, q_width : q_width + k_width].reshape(length, kv_here, HD), positions
    ).astype(jnp.bfloat16)
    value_block = projected[:, q_width + k_width :].reshape(length, kv_here, HD).astype(jnp.bfloat16)
    return attend(queries, key_block, value_block)


def solution(mesh):
    split = Mesh(mesh.devices.reshape(2, mesh.shape["dp"] // 4, 2, 2, 4), ALL)
    in_specs = (P(DP, MP), P(MP, DP), P(), P(DP, MP), P(DP, MP), P(DP, MP))
    return jax.shard_map(
        per_device, mesh=split, in_specs=in_specs, out_specs=P(DP, MP), check_vma=False
    )
```
